32 devices in a mesh: layer: 8 (over y, x, core), dp: 4 (over z).
Axes of the slice: x: 2, y: 2, z: 4, core: 2. Of those that a mesh axis runs over, the one named last changes fastest.
Arguments:
- weights: bfloat16 [32, 512, 512], P('layer', 'dp'), may hold values from -0.25 to 0.25
- biases: float32 [32, 512], P('layer'), may hold values from -3 to 3
- guesses: float32 [8, 2048, 512], P('layer', 'dp'), may hold values from -6 to 6
Outputs:
- states: bfloat16 [32, 2048, 512], P('layer', 'dp')
The draws below stay inside these ranges and needn't reach their ends.
All inputs are finite; a program needn't handle non-finite values.
Results may differ from the reference program's by a relative error of at most 0.0041.
Values may be sent and summed in bfloat16 or wider, within the bound.
No kernel may reach another device: no remote copies, remote signals or barrier semaphores. Data moves between devices by JAX's collectives and lax.ppermute only.
A program may use at most 64 MiB of HBM per device.

```python
import jax
import jax.numpy as jnp
from jax import lax

D = 512
L_DEV = 4
GROUP = 4
BLOCKS = 8
LAYERS = 32
BATCH = 2048
N_LAYER = 8


def levels(own_key, shape, shards, low, top_value):
    def one(axis_at, shards_of):
        steps = jax.random.uniform(jax.random.fold_in(jax.random.fold_in(own_key, 6), axis_at), (shards_of,), jnp.float32, low / len(shards), top_value / len(shards))
        return jnp.repeat(jnp.exp(steps), shape[axis_at] // shards_of).reshape((-1,) + (1,) * (len(shape) - axis_at - 1))

    level = one(*shards[0])
    for cut in shards[1:]:
        level = level * one(*cut)
    return level


def normal_values(key, extent, width, limit, shards=(), dtype=jnp.bfloat16):
    array = jax.random.normal(key, extent, jnp.float32) * width
    if len(shards) > 0:
        array = levels(key, extent, shards, -0.22, 0.18) * array
    return jnp.clip(array, min=-limit, max=limit).astype(dtype)


def setup_inputs(seed: int = 0) -> dict:
    key_of = jax.random.split(jax.random.key(seed), 4)
    return {
        "weights": normal_values(key_of[0], (LAYERS, D, D), D ** -0.5, 0.25, ((0, 8), (1, 4))),
        "biases": normal_values(key_of[1], (LAYERS, D), 0.5, 3.0, ((0, 8),), jnp.float32),
        "guesses": normal_values(key_of[2], (BLOCKS, BATCH, D), 1.0, 6.0, ((0, 8), (1, 4)), jnp.float32),
    }


def advance(states_in, weight_mat, bias_row, step_width):
    preact = jnp.dot(states_in.astype(jnp.bfloat16), weight_mat, preferred_element_type=jnp.float32)
    return states_in + step_width * jnp.tanh(preact + bias_row)


def advance_each(states_in, weight_mats, bias_rows, step_width):
    return lax.map(lambda packed: advance(packed[0], packed[1], packed[2], step_width), (states_in, weight_mats, bias_rows))


def through_block(initial, weight_mats, bias_rows, step_width):
    def layer_step(carry_state, layer_pair):
        next_state = advance(carry_state, layer_pair[0], layer_pair[1], step_width)
        return next_state, next_state
    return lax.scan(layer_step, initial, (weight_mats, bias_rows))


def reference(weights, biases, guesses):
    fine_width = 4.0 / (L_DEV * N_LAYER)
    block_width = L_DEV * fine_width
    group_width = GROUP * block_width
    layer_weights = weights.reshape(N_LAYER, L_DEV, D, D)
    layer_biases = biases.reshape(N_LAYER, L_DEV, D)
    head_weights = layer_weights[:, 0]
    head_biases = layer_biases[:, 0]
    fine_end = lax.map(lambda packed: through_block(packed[0], packed[1], packed[2], fine_width)[0], (guesses, layer_weights, layer_biases))
    coarse_head = advance_each(guesses, head_weights, head_biases, block_width)
    tau_one = jnp.concatenate([jnp.zeros_like(guesses[:1]), fine_end[:-1] - coarse_head[:-1]], axis=0)
    guess_parts = guesses.reshape(N_LAYER, BATCH // GROUP, GROUP, D)
    tau_parts = tau_one.reshape(N_LAYER, BATCH // GROUP, GROUP, D)
    phase_results = []
    for phase in range(GROUP):
        guess_rows = guess_parts[:, :, phase]
        tau_rows = tau_parts[:, :, phase]
        level = guess_rows[0]
        arrival = {}
        for block in range(1, N_LAYER):
            moved = advance(level, head_weights[block - 1], head_biases[block - 1], block_width) + tau_rows[block]
            if (block - phase) % GROUP == 0:
                arrival[block] = moved
                level = guess_rows[block]
            else:
                level = moved
        coarsest = {}
        if phase == 0:
            coarsest[0] = guess_rows[0]
        for block in range(1, N_LAYER):
            if (block - phase) % GROUP == 0:
                if block < GROUP:
                    coarsest[block] = arrival[block]
                else:
                    behind = advance(guess_rows[block - GROUP], head_weights[block - GROUP], head_biases[block - GROUP], group_width)
                    tau_two = arrival[block] - behind
                    coarsest[block] = advance(coarsest[block - GROUP], head_weights[block - GROUP], head_biases[block - GROUP], group_width) + tau_two
        value = guess_rows[0]
        column = [value]
        for block in range(1, N_LAYER):
            if (block - phase) % GROUP == 0:
                value = coarsest[block]
            else:
                value = advance(value, head_weights[block - 1], head_biases[block - 1], block_width) + tau_rows[block]
            column.append(value)
        phase_results.append(jnp.stack(column, axis=0))
    corrected = jnp.stack(phase_results, axis=2).reshape(N_LAYER, BATCH, D)
    states = lax.map(lambda packed: through_block(packed[0], packed[1], packed[2], fine_width)[1], (corrected, layer_weights, layer_biases))
    return states.reshape(LAYERS, BATCH, D).astype(jnp.bfloat16)
```

```python
import functools

import jax
import jax.numpy as jnp
from jax import lax
from jax.experimental import pallas as pl
from jax.experimental.pallas import tpu as pltpu
from jax.sharding import PartitionSpec as P

GROUP = 4
BIAS_ROWS = 16
BF16 = jnp.bfloat16
F32 = jnp.float32
VMEM = pl.BlockSpec(memory_space=pltpu.VMEM)
SMEM = pl.BlockSpec(memory_space=pltpu.SMEM)


def call(kernel, out_shapes, in_specs, args, flops, scratch=(), limit=16 * 2**20):
    nbytes = sum(a.size * a.dtype.itemsize for a in args)
    return pl.pallas_call(
        kernel,
        out_shape=out_shapes,
        in_specs=in_specs,
        out_specs=jax.tree.map(lambda _: VMEM, out_shapes),
        scratch_shapes=list(scratch),
        compiler_params=pltpu.CompilerParams(vmem_limit_bytes=limit),
        cost_estimate=pl.CostEstimate(flops=flops, bytes_accessed=nbytes, transcendentals=0),
    )(*args)


def gather_pieces(piece, axis):
    count = lax.axis_size(axis)
    rank = lax.axis_index(axis)
    if count != 4:
        whole = lax.all_gather(piece, axis, axis=piece.ndim - 2, tiled=True)
        return [whole], jnp.zeros((1,), jnp.int32)
    across = lax.ppermute(piece, axis, [(0, 2), (2, 0), (1, 3), (3, 1)])
    beside = lax.ppermute(piece, axis, [(0, 1), (1, 0), (2, 3), (3, 2)])
    middle = lax.ppermute(piece, axis, [(1, 2), (2, 1)])
    passed = lax.ppermute(across, axis, [(1, 0), (2, 3)])
    rows = piece.shape[-2]
    places = jnp.stack([rank, rank ^ 2, rank ^ 1, rank ^ 3, rank ^ 3]) * rows
    return [piece, across, beside, middle, passed], places.astype(jnp.int32)


def put_pieces(place_ref, pieces, target, lead):
    rows = pieces[0].shape[-2]
    if len(pieces) == 1:
        target[(*lead, pl.ds(0, rows))] = pieces[0][...]
        return
    for number, piece in enumerate(pieces[:3]):
        at = pl.multiple_of(place_ref[number], rows)
        target[(*lead, pl.ds(at, rows))] = piece[...]
    at = pl.multiple_of(place_ref[3], rows)
    target[(*lead, pl.ds(at, rows))] = pieces[3][...] + pieces[4][...]


def head_kernel(place_ref, bias_ref, *refs):
    *pieces, out_ref = refs
    width = out_ref.shape[1]
    put_pieces(place_ref, pieces, out_ref, ())
    bias = bias_ref[0:1, :]
    high = bias.astype(BF16)
    rest = bias - high.astype(F32)
    mid = rest.astype(BF16)
    low = (rest - mid.astype(F32)).astype(BF16)
    row = lax.broadcasted_iota(jnp.int32, (BIAS_ROWS, width), 0)
    tail = jnp.where(row == 0, high, jnp.where(row == 1, mid, jnp.where(row == 2, low, jnp.zeros_like(low))))
    out_ref[pl.ds(width, BIAS_ROWS), :] = tail.astype(BF16)


def fine_kernel(fine_width, place_ref, bias_ref, guess_ref, head_ref, *refs):
    *pieces, tau_ref, rest_ref = refs
    depth = bias_ref.shape[0]
    rows, width = guess_ref.shape
    for layer_no in range(depth - 1):
        put_pieces(place_ref, [p.at[layer_no] for p in pieces], rest_ref, (layer_no,))
    step = rows // 2
    for part in range(2):
        block = pl.ds(part * step, step)
        state = guess_ref[block, :]
        total = None
        for layer_no in range(depth):
            weight = head_ref[pl.ds(0, width), :] if layer_no == 0 else rest_ref[layer_no - 1]
            turn = jnp.tanh(
                jnp.dot(state.astype(BF16), weight, preferred_element_type=F32) + bias_ref[layer_no : layer_no + 1, :]
            )
            if layer_no == 0:
                total = (1.0 - depth) * turn
            else:
                total = total + turn
            if layer_no < depth - 1:
                state = state + fine_width * turn
        tau_ref[block, :] = (fine_width * total).astype(BF16)


def last_kernel(fine_width, rank_ref, bias_ref, guess_ref, head_ref, rest_ref, corrected_ref, out_ref):
    depth = bias_ref.shape[0]
    rows, width = guess_ref.shape
    step = rows // 2
    for part in range(2):
        block = pl.ds(part * step, step)
        state = jnp.where(rank_ref[0] == 0, guess_ref[block, :], corrected_ref[block, :].astype(F32))
        for layer_no in range(depth):
            weight = head_ref[pl.ds(0, width), :] if layer_no == 0 else rest_ref[layer_no - 1]
            turn = jnp.tanh(
                jnp.dot(state.astype(BF16), weight, preferred_element_type=F32) + bias_ref[layer_no : layer_no + 1, :]
            )
            state = state + fine_width * turn
            out_ref[layer_no, block, :] = state.astype(BF16)


def coarse_kernel(block_width, slot_ref, tau_ref, guess_ref, *refs):
    count = tau_ref.shape[0]
    rows, width = tau_ref.shape[1:]
    *heads, out_ref, held, flight = refs
    copies = [
        pltpu.make_async_copy(head, held.at[slot_ref[number]], flight.at[number])
        for number, head in enumerate(heads)
    ]
    for copy in copies:
        copy.start()
    phase = lax.broadcasted_iota(jnp.int32, (rows, width), 0) % GROUP
    for copy in copies:
        copy.wait()

    def step(block, carry):
        level, corrected, jump = carry
        before = block - 1
        both = jnp.concatenate([level, corrected], axis=0)
        tail = held[before, pl.ds(width, BIAS_ROWS), :].astype(F32)
        bias = (tail[0:1, :] + tail[1:2, :]) + tail[2:3, :]
        turn = jnp.tanh(
            jnp.dot(both.astype(BF16), held[before, pl.ds(0, width), :], preferred_element_type=F32) + bias
        )
        turn_level, turn_corrected = turn[:rows], turn[rows:]
        jump = jnp.where(
            phase == before % GROUP,
            (corrected - level) + (GROUP * block_width) * (turn_corrected - turn_level),
            jump,
        )
        tau = tau_ref[before].astype(F32)
        arrival = level + block_width * turn_level + tau
        moved = corrected + block_width * turn_corrected + tau
        own = phase == block % GROUP
        level = jnp.where(own, guess_ref[block].astype(F32), arrival)
        corrected = jnp.where(own, arrival + jump, moved)
        out_ref[block] = corrected.astype(BF16)
        return level, corrected, jump

    first = guess_ref[0].astype(F32)
    out_ref[0] = guess_ref[0].astype(BF16)
    carry = (first, first, jnp.zeros_like(first))
    if count <= 8:
        for block in range(1, count):
            carry = step(block, carry)
    else:
        lax.fori_loop(1, count, step, carry)


def gather_heads(head):
    count = lax.axis_size("layer")
    rank = lax.axis_index("layer")
    chip_bits = [1 << k for k in range(1, count.bit_length() - 1)]
    orders = (chip_bits, chip_bits[::-1])
    held, masks = [head], [(0, 0)]
    for turn_no in range(len(chip_bits)):
        bits = (orders[0][turn_no], orders[1][turn_no])
        pairs = [(source, source ^ bits[source & 1]) for source in range(count)]
        held = held + [lax.ppermute(value, "layer", pairs) for value in held]
        masks = masks + [(even ^ bits[0], odd ^ bits[1]) for even, odd in masks]
    pairs = [(source, source ^ 1) for source in range(count)]
    held = held + [lax.ppermute(value, "layer", pairs) for value in held]
    masks = masks + [(odd ^ 1, even ^ 1) for even, odd in masks]
    slots = jnp.where(rank % 2 == 0, jnp.array([m[0] for m in masks]), jnp.array([m[1] for m in masks])) ^ rank
    return held, slots.astype(jnp.int32)


def per_device(weights, biases, guesses):
    count = lax.axis_size("layer")
    rank = lax.axis_index("layer")
    depth, _, width = weights.shape
    rows = guesses.shape[1]
    fine_width = 4.0 / (depth * count)
    block_width = depth * fine_width
    initial = guesses[0]
    part_rows = rows // count

    head_pieces, head_places = gather_pieces(weights[0], "dp")
    rest_pieces, rest_places = gather_pieces(weights[1:], "dp")
    head = call(
        head_kernel,
        jax.ShapeDtypeStruct((width + BIAS_ROWS, width), BF16),
        [SMEM] + [VMEM] * (1 + len(head_pieces)),
        (head_places, biases, *head_pieces),
        1 << 20,
    )
    guess_parts = lax.all_to_all(initial.astype(BF16).reshape(count, part_rows, width), "layer", 0, 0)
    heads, slots = gather_heads(head)

    tau, rest = call(
        functools.partial(fine_kernel, fine_width),
        (
            jax.ShapeDtypeStruct((rows, width), BF16),
            jax.ShapeDtypeStruct((depth - 1, width, width), BF16),
        ),
        [SMEM] + [VMEM] * (3 + len(rest_pieces)),
        (rest_places, biases, initial, head, *rest_pieces),
        2 * depth * rows * width * width,
    )
    tau_parts = lax.all_to_all(tau.reshape(count, part_rows, width), "layer", 0, 0)
    corrected_parts = call(
        functools.partial(coarse_kernel, block_width),
        jax.ShapeDtypeStruct((count, part_rows, width), BF16),
        [SMEM, VMEM, VMEM] + [pl.BlockSpec(memory_space=pl.ANY)] * count,
        (slots, tau_parts, guess_parts, *heads),
        4 * count * part_rows * width * width,
        (pltpu.VMEM((count, width + BIAS_ROWS, width), BF16), pltpu.SemaphoreType.DMA((count,))),
        limit=2 * count * (width + BIAS_ROWS) * width + 8 * 2**20,
    )
    corrected = lax.all_to_all(corrected_parts, "layer", 0, 0)
    return call(
        functools.partial(last_kernel, fine_width),
        jax.ShapeDtypeStruct((depth, rows, width), BF16),
        [SMEM] + [VMEM] * 5,
        (rank.reshape(1).astype(jnp.int32), biases, initial, head, rest, corrected.reshape(rows, width)),
        2 * depth * rows * width * width,
    )


def solution(mesh):
    in_specs = (P("layer", "dp", None), P("layer", None), P("layer", "dp", None))
    out_specs = P("layer", "dp", None)
    return jax.shard_map(
        per_device, mesh=mesh, in_specs=in_specs, out_specs=out_specs, check_vma=False
    )
```

```python
import functools

import jax
import jax.numpy as jnp
from jax import lax
from jax.experimental import pallas as pl
from jax.experimental.pallas import tpu as pltpu
from jax.sharding import PartitionSpec as P


GROUP = 4
BIAS_ROWS = 16
PIECE_MASKS = (0, 2, 1, 3)
BF16 = jnp.bfloat16
F32 = jnp.float32
VMEM = pl.BlockSpec(memory_space=pltpu.VMEM)
SMEM = pl.BlockSpec(memory_space=pltpu.SMEM)


def call(kernel, out_shapes, in_specs, args, flops, scratch=(), limit=16 * 2**20, out_specs=None):
    nbytes = sum(a.size * a.dtype.itemsize for a in args)
    return pl.pallas_call(
        kernel,
        out_shape=out_shapes,
        in_specs=in_specs,
        out_specs=jax.tree.map(lambda _: VMEM, out_shapes) if out_specs is None else out_specs,
        scratch_shapes=list(scratch),
        compiler_params=pltpu.CompilerParams(vmem_limit_bytes=limit),
        cost_estimate=pl.CostEstimate(flops=flops, bytes_accessed=nbytes, transcendentals=0),
    )(*args)


def gather_pieces(piece, axis):
    if lax.axis_size(axis) != 4:
        return [lax.all_gather(piece, axis, axis=piece.ndim - 2, tiled=True)]
    across = lax.ppermute(piece, axis, [(0, 2), (2, 0), (1, 3), (3, 1)])
    beside = lax.ppermute(piece, axis, [(0, 1), (1, 0), (2, 3), (3, 2)])
    middle = lax.ppermute(piece, axis, [(1, 2), (2, 1)])
    passed = lax.ppermute(across, axis, [(1, 0), (2, 3)])
    return [piece, across, beside, middle, passed]


def put_pieces(own_ref, pieces, target, lead):
    rows = pieces[0].shape[-2]
    if len(pieces) == 1:
        target[(*lead, pl.ds(0, rows))] = pieces[0][...]
        return
    for number, mask in enumerate(PIECE_MASKS):
        at = pl.multiple_of((own_ref[1] ^ mask) * rows, rows)
        value = pieces[number][...]
        if number == 3 and len(pieces) == 5:
            value = value + pieces[4][...]
        target[(*lead, pl.ds(at, rows))] = value


def cut_kernel(weight_ref, bias_in_ref, head_ref, rest_ref, bias_ref, flight):
    copies = [
        pltpu.make_async_copy(weight_ref.at[0], head_ref, flight.at[0]),
        pltpu.make_async_copy(weight_ref.at[pl.ds(1, rest_ref.shape[0])], rest_ref, flight.at[1]),
        pltpu.make_async_copy(bias_in_ref, bias_ref, flight.at[2]),
    ]
    for copy in copies:
        copy.start()
    for copy in copies:
        copy.wait()


def head_kernel(own_ref, bias_ref, *refs):
    *pieces, out_ref = refs
    width = out_ref.shape[1]
    put_pieces(own_ref, pieces, out_ref, ())
    bias = bias_ref[0:1, :]
    high = bias.astype(BF16)
    rest = bias - high.astype(F32)
    mid = rest.astype(BF16)
    low = (rest - mid.astype(F32)).astype(BF16)
    row = lax.broadcasted_iota(jnp.int32, (BIAS_ROWS, width), 0)
    tail = jnp.where(row == 0, high, jnp.where(row == 1, mid, jnp.where(row == 2, low, jnp.zeros_like(low))))
    out_ref[pl.ds(width, BIAS_ROWS), :] = tail.astype(BF16)


def turn_of(state, weight, bias):
    return jnp.tanh(jnp.dot(state.astype(BF16), weight, preferred_element_type=F32) + bias)


def fine_kernel(fine_width, count, own_ref, bias_ref, guess_ref, head_ref, *refs):
    depth = bias_ref.shape[0]
    rows, width = guess_ref.shape
    pieces, tau_refs, rest_ref = refs[: -count - 1], refs[-count - 1 : -1], refs[-1]
    rank = own_ref[0]
    part_rows = rows // count
    half = count // 2
    states, totals = [], [None, None]
    for part in range(2):
        states.append(
            jnp.concatenate(
                [
                    guess_ref[pl.ds(pl.multiple_of((rank ^ mask) * part_rows, part_rows), part_rows), :]
                    for mask in range(part * half, (part + 1) * half)
                ],
                axis=0,
            )
        )
    for layer_no in range(depth):
        if layer_no == 0:
            weight = head_ref[pl.ds(0, width), :]
        else:
            put_pieces(own_ref, [p.at[layer_no - 1] for p in pieces], rest_ref, (layer_no - 1,))
            weight = rest_ref[layer_no - 1]
        bias = bias_ref[layer_no : layer_no + 1, :]
        for part in range(2):
            turn = turn_of(states[part], weight, bias)
            totals[part] = (1.0 - depth) * turn if layer_no == 0 else totals[part] + turn
            if layer_no < depth - 1:
                states[part] = states[part] + fine_width * turn
    for part in range(2):
        tau = (fine_width * totals[part]).astype(BF16)
        for number in range(half):
            tau_refs[part * half + number][...] = tau[number * part_rows : (number + 1) * part_rows]


def last_kernel(fine_width, own_ref, bias_ref, guess_ref, head_ref, rest_ref, *refs):
    *corrected_refs, out_ref, stage, flight = refs
    depth = bias_ref.shape[0]
    rows, width = guess_ref.shape
    count = len(corrected_refs)
    rank = own_ref[0]
    part_rows = rows // count
    half = count // 2
    places = [pl.multiple_of((rank ^ mask) * part_rows, part_rows) for mask in range(count)]
    states, bases, copies = [], [], []
    for part in range(2):
        masks = range(part * half, (part + 1) * half)
        states.append(
            jnp.concatenate(
                [
                    jnp.where(
                        rank == 0,
                        guess_ref[pl.ds(places[mask], part_rows), :],
                        corrected_refs[mask][...].astype(F32),
                    )
                    for mask in masks
                ],
                axis=0,
            )
        )
        bases.append(pl.multiple_of(((rank // half) ^ part) * (rows // 2), rows // 2))
    for layer_no in range(depth):
        weight = head_ref[pl.ds(0, width), :] if layer_no == 0 else rest_ref[layer_no - 1]
        bias = bias_ref[layer_no : layer_no + 1, :]
        for part in range(2):
            states[part] = states[part] + fine_width * turn_of(states[part], weight, bias)
            rounded = states[part].astype(BF16)
            for number in range(half):
                stage[layer_no, pl.ds(places[part * half + number], part_rows), :] = rounded[
                    number * part_rows : (number + 1) * part_rows
                ]
            block = pl.ds(bases[part], rows // 2)
            copy = pltpu.make_async_copy(
                stage.at[layer_no, block], out_ref.at[layer_no, block], flight.at[2 * layer_no + part]
            )
            copy.start()
            copies.append(copy)
    for copy in copies:
        copy.wait()


def hold_kernel(masks, own_ref, *refs):
    *heads, held_ref, flight = refs
    rank = own_ref[0]
    copies = [
        pltpu.make_async_copy(head, held_ref.at[rank ^ jnp.where(rank % 2 == 0, *masks[number])], flight.at[number])
        for number, head in enumerate(heads)
    ]
    for copy in copies:
        copy.start()
    for copy in copies:
        copy.wait()


def split_kernel(own_ref, guess_ref, *out_refs):
    part_rows = out_refs[0].shape[0]
    for mask, out_ref in enumerate(out_refs):
        out_ref[...] = guess_ref[pl.ds(pl.multiple_of((own_ref[0] ^ mask) * part_rows, part_rows), part_rows), :]


def coarse_kernel(block_width, own_ref, held_ref, *refs):
    *refs, tau, guess, found = refs
    count, rows, width = guess.shape
    guess_refs, tau_refs, out_refs = refs[:count], refs[count : 2 * count], refs[2 * count :]
    rank = own_ref[0]
    for mask in range(count):
        guess[rank ^ mask] = guess_refs[mask][...]
        tau[rank ^ mask] = tau_refs[mask][...]
    phase = lax.broadcasted_iota(jnp.int32, (rows, width), 0) % GROUP

    def step(block, carry):
        level, corrected, jump = carry
        before = block - 1
        both = jnp.concatenate([level, corrected], axis=0)
        tail = held_ref[before, pl.ds(width, BIAS_ROWS), :].astype(F32)
        bias = (tail[0:1, :] + tail[1:2, :]) + tail[2:3, :]
        turn = turn_of(both, held_ref[before, pl.ds(0, width), :], bias)
        turn_level, turn_corrected = turn[:rows], turn[rows:]
        jump = jnp.where(
            phase == before % GROUP,
            (corrected - level) + (GROUP * block_width) * (turn_corrected - turn_level),
            jump,
        )
        here = tau[before].astype(F32)
        arrival = level + block_width * turn_level + here
        moved = corrected + block_width * turn_corrected + here
        own = phase == block % GROUP
        level = jnp.where(own, guess[block], arrival)
        corrected = jnp.where(own, arrival + jump, moved)
        found[block] = corrected.astype(BF16)
        return level, corrected, jump

    first = guess[0]
    found[0] = first.astype(BF16)
    carry = (first, first, jnp.zeros_like(first))
    if count <= 8:
        for block in range(1, count):
            carry = step(block, carry)
    else:
        lax.fori_loop(1, count, step, carry)
    for mask in range(count):
        out_refs[mask][...] = found[rank ^ mask]


def gather_heads(head):
    count = lax.axis_size("layer")
    chip_bits = [1 << k for k in range(1, count.bit_length() - 1)]
    orders = (chip_bits, chip_bits[::-1])
    held, masks = [head], [(0, 0)]
    for turn_no in range(len(chip_bits)):
        bits = (orders[0][turn_no], orders[1][turn_no])
        pairs = [(source, source ^ bits[source & 1]) for source in range(count)]
        held = held + [lax.ppermute(value, "layer", pairs) for value in held]
        masks = masks + [(even ^ bits[0], odd ^ bits[1]) for even, odd in masks]
    pairs = [(source, source ^ 1) for source in range(count)]
    held = held + [lax.ppermute(value, "layer", pairs) for value in held]
    masks = masks + [(odd ^ 1, even ^ 1) for even, odd in masks]
    return held, masks


def exchange(values):
    count = len(values)
    return [values[0]] + [
        lax.ppermute(values[mask], "layer", [(source, source ^ mask) for source in range(count)])
        for mask in range(1, count)
    ]


def per_device(weights, biases, guesses):
    count = lax.axis_size("layer")
    own = jnp.stack([lax.axis_index("layer"), lax.axis_index("dp")]).astype(jnp.int32)
    depth, _, width = weights.shape
    rows = guesses.shape[1]
    fine_width = 4.0 / (depth * count)
    block_width = depth * fine_width
    initial = guesses[0]
    part_rows = rows // count
    part = jax.ShapeDtypeStruct((part_rows, width), BF16)

    head_own, rest_own, biases = call(
        cut_kernel,
        (
            jax.ShapeDtypeStruct(weights.shape[1:], BF16),
            jax.ShapeDtypeStruct((depth - 1, *weights.shape[1:]), BF16),
            jax.ShapeDtypeStruct(biases.shape, F32),
        ),
        [pl.BlockSpec(memory_space=pltpu.HBM)] * 2,
        (weights, biases),
        1 << 20,
        (pltpu.SemaphoreType.DMA((3,)),),
    )
    head_pieces = gather_pieces(head_own, "dp")
    rest_pieces = gather_pieces(rest_own, "dp")
    guess_parts = call(
        split_kernel,
        (jax.ShapeDtypeStruct((part_rows, width), F32),) * count,
        [SMEM, VMEM],
        (own, initial),
        1 << 20,
    )
    guess_parts = exchange(guess_parts)
    head = call(
        head_kernel,
        jax.ShapeDtypeStruct((width + BIAS_ROWS, width), BF16),
        [SMEM] + [VMEM] * (1 + len(head_pieces)),
        (own, biases, *head_pieces),
        1 << 20,
    )
    heads, masks = gather_heads(head)

    *tau, rest = call(
        functools.partial(fine_kernel, fine_width, count),
        (part,) * count + (jax.ShapeDtypeStruct((depth - 1, width, width), BF16),),
        [SMEM] + [VMEM] * (3 + len(rest_pieces)),
        (own, biases, initial, head, *rest_pieces),
        2 * depth * rows * width * width,
    )
    tau = exchange(tau)
    held_size = 2 * count * (width + BIAS_ROWS) * width
    held = call(
        functools.partial(hold_kernel, masks),
        jax.ShapeDtypeStruct((count, width + BIAS_ROWS, width), BF16),
        [SMEM] + [pl.BlockSpec(memory_space=pl.ANY)] * count,
        (own, *heads),
        1 << 28,
        (pltpu.SemaphoreType.DMA((count,)),),
        limit=held_size + 2 * 2**20,
    )
    corrected = call(
        functools.partial(coarse_kernel, block_width),
        (part,) * count,
        [SMEM] + [VMEM] * (1 + 2 * count),
        (own, held, *guess_parts, *tau),
        4 * rows * width * width,
        tuple(pltpu.VMEM((count, part_rows, width), kind) for kind in (BF16, F32, BF16)),
        limit=held_size + 12 * 2**20,
    )
    corrected = exchange(corrected)
    return call(
        functools.partial(last_kernel, fine_width),
        jax.ShapeDtypeStruct((depth, rows, width), BF16),
        [SMEM] + [VMEM] * (4 + count),
        (own, biases, initial, head, rest, *corrected),
        2 * depth * rows * width * width,
        (pltpu.VMEM((depth, rows, width), BF16), pltpu.SemaphoreType.DMA((2 * depth,))),
        out_specs=pl.BlockSpec(memory_space=pl.ANY),
    )


def solution(mesh):
    in_specs = (P("layer", "dp", None), P("layer", None), P("layer", "dp", None))
    out_specs = P("layer", "dp", None)

    return jax.shard_map(per_device, mesh=mesh, in_specs=in_specs, out_specs=out_specs, check_vma=False)
```

```python
import functools

import jax
import jax.numpy as jnp
from jax import lax
from jax.experimental import pallas as pl
from jax.experimental.pallas import tpu as pltpu
from jax.sharding import PartitionSpec as P


GROUP = 4
BIAS_ROWS = 16
PIECE_MASKS = (0, 2, 1, 3)
BF16 = jnp.bfloat16
F32 = jnp.float32
VMEM = pl.BlockSpec(memory_space=pltpu.VMEM)
SMEM = pl.BlockSpec(memory_space=pltpu.SMEM)


def call(kernel, out_shapes, in_specs, args, flops, scratch=(), limit=16 * 2**20, out_specs=None):
    nbytes = sum(a.size * a.dtype.itemsize for a in args)
    return pl.pallas_call(
        kernel,
        out_shape=out_shapes,
        in_specs=in_specs,
        out_specs=jax.tree.map(lambda _: VMEM, out_shapes) if out_specs is None else out_specs,
        scratch_shapes=list(scratch),
        compiler_params=pltpu.CompilerParams(vmem_limit_bytes=limit),
        cost_estimate=pl.CostEstimate(flops=flops, bytes_accessed=nbytes, transcendentals=0),
    )(*args)


def gather_whole(piece, axis):
    return [lax.all_gather(piece, axis, axis=piece.ndim - 2, tiled=True)]


def gather_direct(piece, axis):
    if lax.axis_size(axis) != 4:
        return gather_whole(piece, axis)
    return [piece] + [
        lax.ppermute(piece, axis, [(source, source ^ mask) for source in range(4)]) for mask in PIECE_MASKS[1:]
    ]


def gather_passed(piece, axis):
    if lax.axis_size(axis) != 4:
        return gather_whole(piece, axis)
    across = lax.ppermute(piece, axis, [(0, 2), (2, 0), (1, 3), (3, 1)])
    beside = lax.ppermute(piece, axis, [(0, 1), (1, 0), (2, 3), (3, 2)])
    middle = lax.ppermute(piece, axis, [(1, 2), (2, 1)])
    passed = lax.ppermute(across, axis, [(1, 0), (2, 3)])
    return [piece, across, beside, middle, passed]


def put_pieces(own_ref, pieces, target, lead):
    rows = pieces[0].shape[-2]
    if len(pieces) == 1:
        target[(*lead, pl.ds(0, rows))] = pieces[0][...]
        return
    for number, mask in enumerate(PIECE_MASKS):
        at = pl.multiple_of((own_ref[1] ^ mask) * rows, rows)
        value = pieces[number][...]
        if number == 3 and len(pieces) == 5:
            value = value + pieces[4][...]
        target[(*lead, pl.ds(at, rows))] = value


def head_kernel(own_ref, bias_ref, *refs):
    *pieces, out_ref = refs
    width = out_ref.shape[1]
    put_pieces(own_ref, pieces, out_ref, ())
    bias = bias_ref[0:1, :]
    high = bias.astype(BF16)
    rest = bias - high.astype(F32)
    mid = rest.astype(BF16)
    low = (rest - mid.astype(F32)).astype(BF16)
    row = lax.broadcasted_iota(jnp.int32, (BIAS_ROWS, width), 0)
    tail = jnp.where(row == 0, high, jnp.where(row == 1, mid, jnp.where(row == 2, low, jnp.zeros_like(low))))
    out_ref[pl.ds(width, BIAS_ROWS), :] = tail.astype(BF16)


def turn_of(state, weight, bias):
    return jnp.tanh(jnp.dot(state.astype(BF16), weight, preferred_element_type=F32) + bias)


def fine_kernel(fine_width, count, own_ref, bias_ref, guess_ref, head_ref, *refs):
    depth = bias_ref.shape[0]
    rows, width = guess_ref.shape
    pieces, tau_refs, rest_ref = refs[: -count - 1], refs[-count - 1 : -1], refs[-1]
    rank = own_ref[0]
    part_rows = rows // count
    half = count // 2
    states, totals = [], [None, None]
    for part in range(2):
        states.append(
            jnp.concatenate(
                [
                    guess_ref[pl.ds(pl.multiple_of((rank ^ mask) * part_rows, part_rows), part_rows), :]
                    for mask in range(part * half, (part + 1) * half)
                ],
                axis=0,
            )
        )
    for layer_no in range(depth):
        if layer_no == 0:
            weight = head_ref[pl.ds(0, width), :]
        else:
            put_pieces(own_ref, [p.at[layer_no - 1] for p in pieces], rest_ref, (layer_no - 1,))
            weight = rest_ref[layer_no - 1]
        bias = bias_ref[layer_no : layer_no + 1, :]
        for part in range(2):
            turn = turn_of(states[part], weight, bias)
            totals[part] = (1.0 - depth) * turn if layer_no == 0 else totals[part] + turn
            if layer_no < depth - 1:
                states[part] = states[part] + fine_width * turn
    for part in range(2):
        tau = (fine_width * totals[part]).astype(BF16)
        for number in range(half):
            tau_refs[part * half + number][...] = tau[number * part_rows : (number + 1) * part_rows]


def last_kernel(fine_width, own_ref, bias_ref, guess_ref, head_ref, rest_ref, *refs):
    *corrected_refs, out_ref, stage, flight = refs
    depth = bias_ref.shape[0]
    rows, width = guess_ref.shape
    count = len(corrected_refs)
    rank = own_ref[0]
    part_rows = rows // count
    half = count // 2
    places = [pl.multiple_of((rank ^ mask) * part_rows, part_rows) for mask in range(count)]
    states, bases, copies = [], [], []
    for part in range(2):
        masks = range(part * half, (part + 1) * half)
        states.append(
            jnp.concatenate(
                [
                    jnp.where(
                        rank == 0,
                        guess_ref[pl.ds(places[mask], part_rows), :],
                        corrected_refs[mask][...].astype(F32),
                    )
                    for mask in masks
                ],
                axis=0,
            )
        )
        bases.append(pl.multiple_of(((rank // half) ^ part) * (rows // 2), rows // 2))
    for layer_no in range(depth):
        weight = head_ref[pl.ds(0, width), :] if layer_no == 0 else rest_ref[layer_no - 1]
        bias = bias_ref[layer_no : layer_no + 1, :]
        for part in range(2):
            states[part] = states[part] + fine_width * turn_of(states[part], weight, bias)
            rounded = states[part].astype(BF16)
            for number in range(half):
                stage[layer_no, pl.ds(places[part * half + number], part_rows), :] = rounded[
                    number * part_rows : (number + 1) * part_rows
                ]
            block = pl.ds(bases[part], rows // 2)
            copy = pltpu.make_async_copy(
                stage.at[layer_no, block], out_ref.at[layer_no, block], flight.at[2 * layer_no + part]
            )
            copy.start()
            copies.append(copy)
    for copy in copies:
        copy.wait()


def hold_kernel(masks, own_ref, *refs):
    *heads, held_ref, flight = refs
    rank = own_ref[0]
    copies = [
        pltpu.make_async_copy(head, held_ref.at[rank ^ jnp.where(rank % 2 == 0, *masks[number])], flight.at[number])
        for number, head in enumerate(heads)
    ]
    for copy in copies:
        copy.start()
    for copy in copies:
        copy.wait()


def split_kernel(own_ref, guess_ref, *out_refs):
    part_rows = out_refs[0].shape[0]
    for mask, out_ref in enumerate(out_refs):
        out_ref[...] = guess_ref[pl.ds(pl.multiple_of((own_ref[0] ^ mask) * part_rows, part_rows), part_rows), :]


def coarse_kernel(block_width, own_ref, held_ref, *refs):
    *refs, tau, guess, found = refs
    count, rows, width = guess.shape
    guess_refs, tau_refs, out_refs = refs[:count], refs[count : 2 * count], refs[2 * count :]
    rank = own_ref[0]
    for mask in range(count):
        guess[rank ^ mask] = guess_refs[mask][...]
        tau[rank ^ mask] = tau_refs[mask][...]
    phase = lax.broadcasted_iota(jnp.int32, (rows, width), 0) % GROUP

    def step(block, carry):
        level, corrected, jump = carry
        before = block - 1
        both = jnp.concatenate([level, corrected], axis=0)
        tail = held_ref[before, pl.ds(width, BIAS_ROWS), :].astype(F32)
        bias = (tail[0:1, :] + tail[1:2, :]) + tail[2:3, :]
        turn = turn_of(both, held_ref[before, pl.ds(0, width), :], bias)
        turn_level, turn_corrected = turn[:rows], turn[rows:]
        jump = jnp.where(
            phase == before % GROUP,
            (corrected - level) + (GROUP * block_width) * (turn_corrected - turn_level),
            jump,
        )
        here = tau[before].astype(F32)
        arrival = level + block_width * turn_level + here
        moved = corrected + block_width * turn_corrected + here
        own = phase == block % GROUP
        level = jnp.where(own, guess[block], arrival)
        corrected = jnp.where(own, arrival + jump, moved)
        found[block] = corrected.astype(BF16)
        return level, corrected, jump

    first = guess[0]
    found[0] = first.astype(BF16)
    carry = (first, first, jnp.zeros_like(first))
    if count <= 8:
        for block in range(1, count):
            carry = step(block, carry)
    else:
        lax.fori_loop(1, count, step, carry)
    for mask in range(count):
        out_refs[mask][...] = found[rank ^ mask]


def gather_heads(head):
    count = lax.axis_size("layer")
    chip_bits = [1 << k for k in range(1, count.bit_length() - 1)]
    orders = (chip_bits, chip_bits[::-1])
    held, masks = [head], [(0, 0)]
    for turn_no in range(len(chip_bits)):
        bits = (orders[0][turn_no], orders[1][turn_no])
        pairs = [(source, source ^ bits[source & 1]) for source in range(count)]
        held = held + [lax.ppermute(value, "layer", pairs) for value in held]
        masks = masks + [(even ^ bits[0], odd ^ bits[1]) for even, odd in masks]
    pairs = [(source, source ^ 1) for source in range(count)]
    held = held + [lax.ppermute(value, "layer", pairs) for value in held]
    masks = masks + [(odd ^ 1, even ^ 1) for even, odd in masks]
    return held, masks


def exchange(values):
    count = len(values)
    return [values[0]] + [
        lax.ppermute(values[mask], "layer", [(source, source ^ mask) for source in range(count)])
        for mask in range(1, count)
    ]


def per_device(weights, biases, guesses):
    count = lax.axis_size("layer")
    own = jnp.stack([lax.axis_index("layer"), lax.axis_index("dp")]).astype(jnp.int32)
    depth, _, width = weights.shape
    rows = guesses.shape[1]
    fine_width = 4.0 / (depth * count)
    block_width = depth * fine_width
    initial = guesses[0]
    part_rows = rows // count
    part = jax.ShapeDtypeStruct((part_rows, width), BF16)

    head_pieces = gather_direct(weights[0], "dp")
    rest_pieces = gather_passed(weights[1:], "dp")
    guess_parts = call(
        split_kernel,
        (jax.ShapeDtypeStruct((part_rows, width), F32),) * count,
        [SMEM, VMEM],
        (own, initial),
        1 << 20,
    )
    guess_parts = exchange(guess_parts)
    head = call(
        head_kernel,
        jax.ShapeDtypeStruct((width + BIAS_ROWS, width), BF16),
        [SMEM] + [VMEM] * (1 + len(head_pieces)),
        (own, biases, *head_pieces),
        1 << 20,
    )
    heads, masks = gather_heads(head)

    *tau, rest = call(
        functools.partial(fine_kernel, fine_width, count),
        (part,) * count + (jax.ShapeDtypeStruct((depth - 1, width, width), BF16),),
        [SMEM] + [VMEM] * (3 + len(rest_pieces)),
        (own, biases, initial, head, *rest_pieces),
        2 * depth * rows * width * width,
    )
    tau = exchange(tau)
    held_size = 2 * count * (width + BIAS_ROWS) * width
    held = call(
        functools.partial(hold_kernel, masks),
        jax.ShapeDtypeStruct((count, width + BIAS_ROWS, width), BF16),
        [SMEM] + [pl.BlockSpec(memory_space=pl.ANY)] * count,
        (own, *heads),
        1 << 28,
        (pltpu.SemaphoreType.DMA((count,)),),
        limit=held_size + 2 * 2**20,
    )
    corrected = call(
        functools.partial(coarse_kernel, block_width),
        (part,) * count,
        [SMEM] + [VMEM] * (1 + 2 * count),
        (own, held, *guess_parts, *tau),
        4 * rows * width * width,
        tuple(pltpu.VMEM((count, part_rows, width), kind) for kind in (BF16, F32, BF16)),
        limit=held_size + 12 * 2**20,
    )
    corrected = exchange(corrected)
    return call(
        functools.partial(last_kernel, fine_width),
        jax.ShapeDtypeStruct((depth, rows, width), BF16),
        [SMEM] + [VMEM] * (4 + count),
        (own, biases, initial, head, rest, *corrected),
        2 * depth * rows * width * width,
        (pltpu.VMEM((depth, rows, width), BF16), pltpu.SemaphoreType.DMA((2 * depth,))),
        out_specs=pl.BlockSpec(memory_space=pl.ANY),
    )


def solution(mesh):
    in_specs = (P("layer", "dp", None), P("layer", None), P("layer", "dp", None))
    out_specs = P("layer", "dp", None)

    return jax.shard_map(per_device, mesh=mesh, in_specs=in_specs, out_specs=out_specs, check_vma=False)
```

```python
import functools

import jax
import jax.numpy as jnp
from jax import lax
from jax.experimental import pallas as pl
from jax.experimental.pallas import tpu as pltpu
from jax.sharding import PartitionSpec as P


GROUP = 4
BIAS_ROWS = 16
PIECE_MASKS = (0, 2, 1, 3)
BF16 = jnp.bfloat16
F32 = jnp.float32
VMEM = pl.BlockSpec(memory_space=pltpu.VMEM)
SMEM = pl.BlockSpec(memory_space=pltpu.SMEM)


def call(kernel, out_shapes, in_specs, args, flops, scratch=(), limit=16 * 2**20, out_specs=None):
    nbytes = sum(a.size * a.dtype.itemsize for a in args)
    return pl.pallas_call(
        kernel,
        out_shape=out_shapes,
        in_specs=in_specs,
        out_specs=jax.tree.map(lambda _: VMEM, out_shapes) if out_specs is None else out_specs,
        scratch_shapes=list(scratch),
        compiler_params=pltpu.CompilerParams(vmem_limit_bytes=limit),
        cost_estimate=pl.CostEstimate(flops=flops, bytes_accessed=nbytes, transcendentals=0),
    )(*args)


def gather_whole(piece, axis):
    return [lax.all_gather(piece, axis, axis=piece.ndim - 2, tiled=True)]


def gather_direct(piece, axis):
    if lax.axis_size(axis) != 4:
        return gather_whole(piece, axis)
    return [piece] + [
        lax.ppermute(piece, axis, [(source, source ^ mask) for source in range(4)]) for mask in PIECE_MASKS[1:]
    ]


def gather_passed(piece, axis):
    if lax.axis_size(axis) != 4:
        return gather_whole(piece, axis)
    across = lax.ppermute(piece, axis, [(0, 2), (2, 0), (1, 3), (3, 1)])
    beside = lax.ppermute(piece, axis, [(0, 1), (1, 0), (2, 3), (3, 2)])
    middle = lax.ppermute(piece, axis, [(1, 2), (2, 1)])
    passed = lax.ppermute(across, axis, [(1, 0), (2, 3)])
    return [piece, across, beside, middle, passed]


def put_pieces(own_ref, pieces, target, lead):
    rows = pieces[0].shape[-2]
    if len(pieces) == 1:
        target[(*lead, pl.ds(0, rows))] = pieces[0][...]
        return
    for number, mask in enumerate(PIECE_MASKS):
        at = pl.multiple_of((own_ref[1] ^ mask) * rows, rows)
        value = pieces[number][...]
        if number == 3 and len(pieces) == 5:
            value = value + pieces[4][...]
        target[(*lead, pl.ds(at, rows))] = value


def head_kernel(own_ref, bias_ref, *refs):
    *pieces, out_ref = refs
    width = out_ref.shape[1]
    put_pieces(own_ref, pieces, out_ref, ())
    bias = bias_ref[0:1, :]
    high = bias.astype(BF16)
    rest = bias - high.astype(F32)
    mid = rest.astype(BF16)
    low = (rest - mid.astype(F32)).astype(BF16)
    row = lax.broadcasted_iota(jnp.int32, (BIAS_ROWS, width), 0)
    tail = jnp.where(row == 0, high, jnp.where(row == 1, mid, jnp.where(row == 2, low, jnp.zeros_like(low))))
    out_ref[pl.ds(width, BIAS_ROWS), :] = tail.astype(BF16)


def turn_of(state, weight, bias):
    return jnp.tanh(jnp.dot(state.astype(BF16), weight, preferred_element_type=F32) + bias)


def fine_kernel(fine_width, count, own_ref, bias_ref, guess_ref, head_ref, *refs):
    depth = bias_ref.shape[0]
    rows, width = guess_ref.shape
    pieces, tau_refs, rest_ref = refs[: -count - 1], refs[-count - 1 : -1], refs[-1]
    each = len(pieces) // 2
    early = pieces[0].shape[0]
    rank = own_ref[0]
    part_rows = rows // count
    half = count // 2
    states, totals = [], [None, None]
    for part in range(2):
        states.append(
            jnp.concatenate(
                [
                    guess_ref[pl.ds(pl.multiple_of((rank ^ mask) * part_rows, part_rows), part_rows), :]
                    for mask in range(part * half, (part + 1) * half)
                ],
                axis=0,
            )
        )
    for layer_no in range(depth):
        if layer_no == 0:
            weight = head_ref[pl.ds(0, width), :]
        else:
            at = layer_no - 1
            here = [p.at[at] for p in pieces[:each]] if at < early else [p.at[at - early] for p in pieces[each:]]
            put_pieces(own_ref, here, rest_ref, (at,))
            weight = rest_ref[layer_no - 1]
        bias = bias_ref[layer_no : layer_no + 1, :]
        for part in range(2):
            turn = turn_of(states[part], weight, bias)
            totals[part] = (1.0 - depth) * turn if layer_no == 0 else totals[part] + turn
            if layer_no < depth - 1:
                states[part] = states[part] + fine_width * turn
    for part in range(2):
        tau = (fine_width * totals[part]).astype(BF16)
        for number in range(half):
            tau_refs[part * half + number][...] = tau[number * part_rows : (number + 1) * part_rows]


def last_kernel(fine_width, own_ref, bias_ref, guess_ref, head_ref, rest_ref, *refs):
    *corrected_refs, out_ref, stage, flight = refs
    depth = bias_ref.shape[0]
    rows, width = guess_ref.shape
    count = len(corrected_refs)
    rank = own_ref[0]
    part_rows = rows // count
    half = count // 2
    places = [pl.multiple_of((rank ^ mask) * part_rows, part_rows) for mask in range(count)]
    states, bases, copies = [], [], []
    for part in range(2):
        masks = range(part * half, (part + 1) * half)
        states.append(
            jnp.concatenate(
                [
                    jnp.where(
                        rank == 0,
                        guess_ref[pl.ds(places[mask], part_rows), :],
                        corrected_refs[mask][...].astype(F32),
                    )
                    for mask in masks
                ],
                axis=0,
            )
        )
        bases.append(pl.multiple_of(((rank // half) ^ part) * (rows // 2), rows // 2))
    for layer_no in range(depth):
        weight = head_ref[pl.ds(0, width), :] if layer_no == 0 else rest_ref[layer_no - 1]
        bias = bias_ref[layer_no : layer_no + 1, :]
        for part in range(2):
            states[part] = states[part] + fine_width * turn_of(states[part], weight, bias)
            rounded = states[part].astype(BF16)
            for number in range(half):
                stage[layer_no, pl.ds(places[part * half + number], part_rows), :] = rounded[
                    number * part_rows : (number + 1) * part_rows
                ]
            block = pl.ds(bases[part], rows // 2)
            copy = pltpu.make_async_copy(
                stage.at[layer_no, block], out_ref.at[layer_no, block], flight.at[2 * layer_no + part]
            )
            copy.start()
            copies.append(copy)
    for copy in copies:
        copy.wait()


def hold_kernel(masks, own_ref, *refs):
    *heads, held_ref, flight = refs
    rank = own_ref[0]
    copies = [
        pltpu.make_async_copy(head, held_ref.at[rank ^ jnp.where(rank % 2 == 0, *masks[number])], flight.at[number])
        for number, head in enumerate(heads)
    ]
    for copy in copies:
        copy.start()
    for copy in copies:
        copy.wait()


def split_kernel(own_ref, guess_ref, *out_refs):
    part_rows = out_refs[0].shape[0]
    for mask, out_ref in enumerate(out_refs):
        out_ref[...] = guess_ref[pl.ds(pl.multiple_of((own_ref[0] ^ mask) * part_rows, part_rows), part_rows), :]


def coarse_kernel(block_width, own_ref, held_ref, *refs):
    *refs, tau, guess, found = refs
    count, rows, width = guess.shape
    guess_refs, tau_refs, out_refs = refs[:count], refs[count : 2 * count], refs[2 * count :]
    rank = own_ref[0]
    for mask in range(count):
        guess[rank ^ mask] = guess_refs[mask][...]
        tau[rank ^ mask] = tau_refs[mask][...]
    phase = lax.broadcasted_iota(jnp.int32, (rows, width), 0) % GROUP

    def step(block, carry):
        level, corrected, jump = carry
        before = block - 1
        both = jnp.concatenate([level, corrected], axis=0)
        tail = held_ref[before, pl.ds(width, BIAS_ROWS), :].astype(F32)
        bias = (tail[0:1, :] + tail[1:2, :]) + tail[2:3, :]
        turn = turn_of(both, held_ref[before, pl.ds(0, width), :], bias)
        turn_level, turn_corrected = turn[:rows], turn[rows:]
        jump = jnp.where(
            phase == before % GROUP,
            (corrected - level) + (GROUP * block_width) * (turn_corrected - turn_level),
            jump,
        )
        here = tau[before].astype(F32)
        arrival = level + block_width * turn_level + here
        moved = corrected + block_width * turn_corrected + here
        own = phase == block % GROUP
        level = jnp.where(own, guess[block], arrival)
        corrected = jnp.where(own, arrival + jump, moved)
        found[block] = corrected.astype(BF16)
        return level, corrected, jump

    first = guess[0]
    found[0] = first.astype(BF16)
    carry = (first, first, jnp.zeros_like(first))
    if count <= 8:
        for block in range(1, count):
            carry = step(block, carry)
    else:
        lax.fori_loop(1, count, step, carry)
    for mask in range(count):
        out_refs[mask][...] = found[rank ^ mask]


def gather_heads(head):
    count = lax.axis_size("layer")
    chip_bits = [1 << k for k in range(1, count.bit_length() - 1)]
    orders = (chip_bits, chip_bits[::-1])
    held, masks = [head], [(0, 0)]
    for turn_no in range(len(chip_bits)):
        bits = (orders[0][turn_no], orders[1][turn_no])
        pairs = [(source, source ^ bits[source & 1]) for source in range(count)]
        held = held + [lax.ppermute(value, "layer", pairs) for value in held]
        masks = masks + [(even ^ bits[0], odd ^ bits[1]) for even, odd in masks]
    pairs = [(source, source ^ 1) for source in range(count)]
    held = held + [lax.ppermute(value, "layer", pairs) for value in held]
    masks = masks + [(odd ^ 1, even ^ 1) for even, odd in masks]
    return held, masks


def exchange(values):
    count = len(values)
    return [values[0]] + [
        lax.ppermute(values[mask], "layer", [(source, source ^ mask) for source in range(count)])
        for mask in range(1, count)
    ]


def per_device(weights, biases, guesses):
    count = lax.axis_size("layer")
    own = jnp.stack([lax.axis_index("layer"), lax.axis_index("dp")]).astype(jnp.int32)
    depth, _, width = weights.shape
    rows = guesses.shape[1]
    fine_width = 4.0 / (depth * count)
    block_width = depth * fine_width
    initial = guesses[0]
    part_rows = rows // count
    part = jax.ShapeDtypeStruct((part_rows, width), BF16)

    head_pieces = gather_direct(weights[0], "dp")
    rest_pieces = gather_passed(weights[1:-1], "dp") + gather_passed(weights[-1:], "dp")
    guess_parts = call(
        split_kernel,
        (jax.ShapeDtypeStruct((part_rows, width), F32),) * count,
        [SMEM, VMEM],
        (own, initial),
        1 << 20,
    )
    guess_parts = exchange(guess_parts)
    head = call(
        head_kernel,
        jax.ShapeDtypeStruct((width + BIAS_ROWS, width), BF16),
        [SMEM] + [VMEM] * (1 + len(head_pieces)),
        (own, biases, *head_pieces),
        1 << 20,
    )
    heads, masks = gather_heads(head)

    *tau, rest = call(
        functools.partial(fine_kernel, fine_width, count),
        (part,) * count + (jax.ShapeDtypeStruct((depth - 1, width, width), BF16),),
        [SMEM] + [VMEM] * (3 + len(rest_pieces)),
        (own, biases, initial, head, *rest_pieces),
        2 * depth * rows * width * width,
    )
    tau = exchange(tau)
    held_size = 2 * count * (width + BIAS_ROWS) * width
    held = call(
        functools.partial(hold_kernel, masks),
        jax.ShapeDtypeStruct((count, width + BIAS_ROWS, width), BF16),
        [SMEM] + [pl.BlockSpec(memory_space=pl.ANY)] * count,
        (own, *heads),
        1 << 28,
        (pltpu.SemaphoreType.DMA((count,)),),
        limit=held_size + 2 * 2**20,
    )
    corrected = call(
        functools.partial(coarse_kernel, block_width),
        (part,) * count,
        [SMEM] + [VMEM] * (1 + 2 * count),
        (own, held, *guess_parts, *tau),
        4 * rows * width * width,
        tuple(pltpu.VMEM((count, part_rows, width), kind) for kind in (BF16, F32, BF16)),
        limit=held_size + 12 * 2**20,
    )
    corrected = exchange(corrected)
    return call(
        functools.partial(last_kernel, fine_width),
        jax.ShapeDtypeStruct((depth, rows, width), BF16),
        [SMEM] + [VMEM] * (4 + count),
        (own, biases, initial, head, rest, *corrected),
        2 * depth * rows * width * width,
        (pltpu.VMEM((depth, rows, width), BF16), pltpu.SemaphoreType.DMA((2 * depth,))),
        out_specs=pl.BlockSpec(memory_space=pl.ANY),
    )


def solution(mesh):
    in_specs = (P("layer", "dp", None), P("layer", None), P("layer", "dp", None))
    out_specs = P("layer", "dp", None)

    return jax.shard_map(per_device, mesh=mesh, in_specs=in_specs, out_specs=out_specs, check_vma=False)
```

```python
import functools

import jax
import jax.numpy as jnp
from jax import lax
from jax.experimental import pallas as pl
from jax.experimental.pallas import tpu as pltpu
from jax.sharding import PartitionSpec as P


GROUP = 4
BIAS_ROWS = 16
ROW_GROUPS = 2
PIECE_MASKS = (0, 2, 1, 3)
BF16 = jnp.bfloat16
F32 = jnp.float32
VMEM = pl.BlockSpec(memory_space=pltpu.VMEM)
SMEM = pl.BlockSpec(memory_space=pltpu.SMEM)


def call(kernel, out_shapes, in_specs, args, flops, scratch=(), limit=16 * 2**20, out_specs=None):
    nbytes = sum(a.size * a.dtype.itemsize for a in args)
    return pl.pallas_call(
        kernel,
        out_shape=out_shapes,
        in_specs=in_specs,
        out_specs=jax.tree.map(lambda _: VMEM, out_shapes) if out_specs is None else out_specs,
        scratch_shapes=list(scratch),
        compiler_params=pltpu.CompilerParams(vmem_limit_bytes=limit),
        cost_estimate=pl.CostEstimate(flops=flops, bytes_accessed=nbytes, transcendentals=0),
    )(*args)


def gather_whole(piece, axis):
    return [lax.all_gather(piece, axis, axis=piece.ndim - 2, tiled=True)]


def gather_direct(piece, axis):
    if lax.axis_size(axis) != 4:
        return gather_whole(piece, axis)
    return [piece] + [
        lax.ppermute(piece, axis, [(source, source ^ mask) for source in range(4)]) for mask in PIECE_MASKS[1:]
    ]


def gather_passed(piece, axis):
    if lax.axis_size(axis) != 4:
        return gather_whole(piece, axis)
    across = lax.ppermute(piece, axis, [(0, 2), (2, 0), (1, 3), (3, 1)])
    beside = lax.ppermute(piece, axis, [(0, 1), (1, 0), (2, 3), (3, 2)])
    middle = lax.ppermute(piece, axis, [(1, 2), (2, 1)])
    passed = lax.ppermute(across, axis, [(1, 0), (2, 3)])
    return [piece, across, beside, middle, passed]


def put_pieces(own_ref, pieces, target, lead):
    rows = pieces[0].shape[-2]
    if len(pieces) == 1:
        target[(*lead, pl.ds(0, rows))] = pieces[0][...]
        return
    for number, mask in enumerate(PIECE_MASKS):
        at = pl.multiple_of((own_ref[1] ^ mask) * rows, rows)
        value = pieces[number][...]
        if number == 3 and len(pieces) == 5:
            value = value + pieces[4][...]
        target[(*lead, pl.ds(at, rows))] = value


def head_kernel(own_ref, bias_ref, *refs):
    *pieces, out_ref = refs
    width = out_ref.shape[1]
    put_pieces(own_ref, pieces, out_ref, ())
    bias = bias_ref[0:1, :]
    high = bias.astype(BF16)
    rest = bias - high.astype(F32)
    mid = rest.astype(BF16)
    low = (rest - mid.astype(F32)).astype(BF16)
    row = lax.broadcasted_iota(jnp.int32, (BIAS_ROWS, width), 0)
    tail = jnp.where(row == 0, high, jnp.where(row == 1, mid, jnp.where(row == 2, low, jnp.zeros_like(low))))
    out_ref[pl.ds(width, BIAS_ROWS), :] = tail.astype(BF16)


def turn_of(state, weight, bias):
    return jnp.tanh(jnp.dot(state.astype(BF16), weight, preferred_element_type=F32) + bias)


def fine_kernel(fine_width, count, own_ref, bias_ref, head_ref, *refs):
    guess_refs, (*pieces, state_ref, defect_ref, early_ref) = refs[:count], refs[count:]
    depth = bias_ref.shape[0]
    rows, width = state_ref.shape
    half = count // 2
    states = [jnp.concatenate([r[...] for r in guess_refs[k * half : (k + 1) * half]], axis=0) for k in range(2)]
    totals = [None, None]
    for layer_no in range(depth - 1):
        if layer_no == 0:
            weight = head_ref[pl.ds(0, width), :]
        else:
            put_pieces(own_ref, [p.at[layer_no - 1] for p in pieces], early_ref, (layer_no - 1,))
            weight = early_ref[layer_no - 1]
        bias = bias_ref[layer_no : layer_no + 1, :]
        for part in range(2):
            turn = turn_of(states[part], weight, bias)
            totals[part] = (1.0 - depth) * turn if layer_no == 0 else totals[part] + turn
            states[part] = states[part] + fine_width * turn
    for part in range(2):
        block = pl.ds(part * (rows // 2), rows // 2)
        state_ref[block, :] = states[part].astype(BF16)
        defect_ref[block, :] = totals[part]


def defect_kernel(fine_width, count, own_ref, bias_ref, state_ref, defect_ref, *refs):
    pieces, tau_refs, late_ref = refs[: -count - 1], refs[-count - 1 : -1], refs[-1]
    depth = bias_ref.shape[0]
    rows = state_ref.shape[0]
    part_rows = rows // count
    half = count // 2
    put_pieces(own_ref, [p.at[0] for p in pieces], late_ref, (0,))
    for part in range(2):
        block = pl.ds(part * (rows // 2), rows // 2)
        turn = turn_of(state_ref[block, :], late_ref[0], bias_ref[depth - 1 : depth, :])
        tau = (fine_width * (defect_ref[block, :] + turn)).astype(BF16)
        for number in range(half):
            tau_refs[part * half + number][...] = tau[number * part_rows : (number + 1) * part_rows]


def last_kernel(fine_width, own_ref, bias_ref, head_ref, early_ref, late_ref, *refs):
    *refs, out_ref, stage, flight = refs
    guess_refs, corrected_refs = refs[: len(refs) // 2], refs[len(refs) // 2 :]
    depth, width = bias_ref.shape
    groups = stage.shape[1]
    each = len(corrected_refs) // groups
    rank = own_ref[0]
    part_rows = stage.shape[2] // each
    states, copies = [], []
    for group in range(groups):
        values = []
        for number in range(group * each, (group + 1) * each):
            values.append(
                jnp.where(rank == 0, guess_refs[number][...], corrected_refs[number][...].astype(F32))
            )
        states.append(jnp.concatenate(values, axis=0))
    for layer_no in range(depth):
        if layer_no == 0:
            weight = head_ref[pl.ds(0, width), :]
        else:
            weight = early_ref[layer_no - 1] if layer_no < depth - 1 else late_ref[0]
        bias = bias_ref[layer_no : layer_no + 1, :]
        for group in range(groups):
            states[group] = states[group] + fine_width * turn_of(states[group], weight, bias)
            rounded = states[group].astype(BF16)
            first = rank ^ (group * each)
            for number in range(each):
                slot = pl.multiple_of(((first ^ number) % each) * part_rows, part_rows)
                stage[layer_no, group, pl.ds(slot, part_rows), :] = rounded[
                    number * part_rows : (number + 1) * part_rows
                ]
            base = pl.multiple_of((first // each) * (each * part_rows), each * part_rows)
            copy = pltpu.make_async_copy(
                stage.at[layer_no, group],
                out_ref.at[layer_no, pl.ds(base, each * part_rows)],
                flight.at[groups * layer_no + group],
            )
            copy.start()
            copies.append(copy)
    for copy in copies:
        copy.wait()


def hold_kernel(masks, own_ref, *refs):
    *heads, held_ref, flight = refs
    rank = own_ref[0]
    copies = [
        pltpu.make_async_copy(head, held_ref.at[rank ^ jnp.where(rank % 2 == 0, *masks[number])], flight.at[number])
        for number, head in enumerate(heads)
    ]
    for copy in copies:
        copy.start()
    for copy in copies:
        copy.wait()


def split_kernel(own_ref, guess_ref, *out_refs):
    part_rows = out_refs[0].shape[0]
    for mask, out_ref in enumerate(out_refs):
        out_ref[...] = guess_ref[pl.ds(pl.multiple_of((own_ref[0] ^ mask) * part_rows, part_rows), part_rows), :]


def coarse_kernel(block_width, own_ref, held_ref, *refs):
    *refs, tau, guess, found = refs
    count, rows, width = guess.shape
    guess_refs, tau_refs, out_refs = refs[:count], refs[count : 2 * count], refs[2 * count :]
    rank = own_ref[0]
    for mask in range(count):
        guess[rank ^ mask] = guess_refs[mask][...]
        tau[rank ^ mask] = tau_refs[mask][...]
    phase = lax.broadcasted_iota(jnp.int32, (rows, width), 0) % GROUP

    def step(block, carry):
        level, corrected, jump = carry
        before = block - 1
        both = jnp.concatenate([level, corrected], axis=0)
        tail = held_ref[before, pl.ds(width, BIAS_ROWS), :].astype(F32)
        bias = (tail[0:1, :] + tail[1:2, :]) + tail[2:3, :]
        turn = turn_of(both, held_ref[before, pl.ds(0, width), :], bias)
        turn_level, turn_corrected = turn[:rows], turn[rows:]
        jump = jnp.where(
            phase == before % GROUP,
            (corrected - level) + (GROUP * block_width) * (turn_corrected - turn_level),
            jump,
        )
        here = tau[before].astype(F32)
        arrival = level + block_width * turn_level + here
        moved = corrected + block_width * turn_corrected + here
        own = phase == block % GROUP
        level = jnp.where(own, guess[block], arrival)
        corrected = jnp.where(own, arrival + jump, moved)
        found[block] = corrected.astype(BF16)
        return level, corrected, jump

    first = guess[0]
    found[0] = first.astype(BF16)
    carry = (first, first, jnp.zeros_like(first))
    if count <= 8:
        for block in range(1, count):
            carry = step(block, carry)
    else:
        lax.fori_loop(1, count, step, carry)
    for mask in range(count):
        out_refs[mask][...] = found[rank ^ mask]


def gather_heads(head):
    count = lax.axis_size("layer")
    chip_bits = [1 << k for k in range(1, count.bit_length() - 1)]
    orders = (chip_bits, chip_bits[::-1])
    held, masks = [head], [(0, 0)]
    for turn_no in range(len(chip_bits)):
        bits = (orders[0][turn_no], orders[1][turn_no])
        pairs = [(source, source ^ bits[source & 1]) for source in range(count)]
        held = held + [lax.ppermute(value, "layer", pairs) for value in held]
        masks = masks + [(even ^ bits[0], odd ^ bits[1]) for even, odd in masks]
    pairs = [(source, source ^ 1) for source in range(count)]
    held = held + [lax.ppermute(value, "layer", pairs) for value in held]
    masks = masks + [(odd ^ 1, even ^ 1) for even, odd in masks]
    return held, masks


def exchange(values):
    count = len(values)
    return [values[0]] + [
        lax.ppermute(values[mask], "layer", [(source, source ^ mask) for source in range(count)])
        for mask in range(1, count)
    ]


def per_device(weights, biases, guesses):
    count = lax.axis_size("layer")
    own = jnp.stack([lax.axis_index("layer"), lax.axis_index("dp")]).astype(jnp.int32)
    depth, _, width = weights.shape
    rows = guesses.shape[1]
    fine_width = 4.0 / (depth * count)
    block_width = depth * fine_width
    part_rows = rows // count
    part = jax.ShapeDtypeStruct((part_rows, width), BF16)

    head_pieces = gather_direct(weights[0], "dp")
    early_pieces = gather_passed(weights[1:-1], "dp")
    late_pieces = gather_passed(weights[-1:], "dp")
    guess_parts = call(
        split_kernel,
        (jax.ShapeDtypeStruct((part_rows, width), F32),) * count,
        [SMEM, VMEM],
        (own, guesses[0]),
        1 << 20,
    )
    far_parts = exchange(guess_parts)
    head = call(
        head_kernel,
        jax.ShapeDtypeStruct((width + BIAS_ROWS, width), BF16),
        [SMEM] + [VMEM] * (1 + len(head_pieces)),
        (own, biases, *head_pieces),
        1 << 20,
    )
    heads, masks = gather_heads(head)

    state, defect, early = call(
        functools.partial(fine_kernel, fine_width, count),
        (
            jax.ShapeDtypeStruct((rows, width), BF16),
            jax.ShapeDtypeStruct((rows, width), F32),
            jax.ShapeDtypeStruct((depth - 2, width, width), BF16),
        ),
        [SMEM] + [VMEM] * (2 + count + len(early_pieces)),
        (own, biases, head, *guess_parts, *early_pieces),
        2 * (depth - 1) * rows * width * width,
    )
    *tau, late = call(
        functools.partial(defect_kernel, fine_width, count),
        (part,) * count + (jax.ShapeDtypeStruct((1, width, width), BF16),),
        [SMEM] + [VMEM] * (3 + len(late_pieces)),
        (own, biases, state, defect, *late_pieces),
        2 * rows * width * width,
    )
    tau = exchange(tau)
    held_size = 2 * count * (width + BIAS_ROWS) * width
    held = call(
        functools.partial(hold_kernel, masks),
        jax.ShapeDtypeStruct((count, width + BIAS_ROWS, width), BF16),
        [SMEM] + [pl.BlockSpec(memory_space=pl.ANY)] * count,
        (own, *heads),
        1 << 28,
        (pltpu.SemaphoreType.DMA((count,)),),
        limit=held_size + 2 * 2**20,
    )
    corrected = call(
        functools.partial(coarse_kernel, block_width),
        (part,) * count,
        [SMEM] + [VMEM] * (1 + 2 * count),
        (own, held, *far_parts, *tau),
        4 * rows * width * width,
        tuple(pltpu.VMEM((count, part_rows, width), kind) for kind in (BF16, F32, BF16)),
        limit=held_size + 12 * 2**20,
    )
    corrected = exchange(corrected)
    return call(
        functools.partial(last_kernel, fine_width),
        jax.ShapeDtypeStruct((depth, rows, width), BF16),
        [SMEM] + [VMEM] * (4 + 2 * count),
        (own, biases, head, early, late, *guess_parts, *corrected),
        2 * depth * rows * width * width,
        (
            pltpu.VMEM((depth, ROW_GROUPS, rows // ROW_GROUPS, width), BF16),
            pltpu.SemaphoreType.DMA((depth * ROW_GROUPS,)),
        ),
        out_specs=pl.BlockSpec(memory_space=pl.ANY),
    )


def solution(mesh):
    in_specs = (P("layer", "dp", None), P("layer", None), P("layer", "dp", None))
    out_specs = P("layer", "dp", None)

    return jax.shard_map(per_device, mesh=mesh, in_specs=in_specs, out_specs=out_specs, check_vma=False)
```
